32 devices in a mesh: space: 8 (over z, x), tm: 4 (over y, core).
Axes of the slice: x: 2, y: 2, z: 4, core: 2. Of those that a mesh axis runs over, the one named last changes fastest.
Arguments:
- snapshots: float32 [16384, 4096], P('space', 'tm'), may hold values from -3000 to 3000, as said below
- sketch: float32 [4096, 256], P('tm'), may hold values from -6 to 6
Outputs:
- refined: float32 [16384, 256], P('space')
- cosample: float32 [4096, 256], P('tm')
The draws below stay inside these ranges and needn't reach their ends.
Inputs may be any that keep to these rules, and one draw needn't show every extreme that they name: `snapshots`: float32 snapshot values.
All inputs are finite; a program needn't handle non-finite values.
Results may differ from the reference program's by a relative error of at most 0.000071.
Values sent between devices are 32-bit elements; how exact they have to be, the bound alone decides.
No kernel may reach another device: no remote copies, remote signals or barrier semaphores. Data moves between devices by JAX's collectives and lax.ppermute only.
A program may use at most 64 MiB of HBM per device.

```python
import jax
import jax.numpy as jnp
from jax import lax

K = 256
POINTS = 16384
TIMES = 4096


def draw_snapshots(key, part):
    first, second, third = jax.random.split(key, 3)
    base = jnp.clip(jax.random.normal(first, (POINTS, TIMES), jnp.float32), -6.0, 6.0)
    cols = jnp.exp(jax.random.uniform(third, (1, TIMES), jnp.float32, 0.0, 2.3))
    rows = jnp.exp(jax.random.uniform(second, (POINTS, 1), jnp.float32, 0.0, 2.3))
    return base * rows * cols


def level_of(rng, extent, pieces, low, largest):
    gain, own = 1.0, jax.random.fold_in(rng, 6)
    for axis_at, shards_of in pieces:
        draws = jnp.exp(jax.random.uniform(jax.random.fold_in(own, axis_at), (shards_of,), jnp.float32, low / len(pieces), largest / len(pieces)))
        gain = gain * jnp.repeat(draws, extent[axis_at] // shards_of).reshape([-1 if axis == axis_at else 1 for axis in range(len(extent))])
    return gain


def gaussian(rng, extent, scale, limit, cuts=(), held_as=jnp.bfloat16):
    result = scale * jax.random.normal(rng, extent, jnp.float32)
    if cuts:
        result = result * level_of(rng, extent, cuts, -0.22, 0.18)
    return jnp.clip(result, -limit, limit).astype(held_as)


def setup_inputs(seed: int = 0) -> dict:
    seeds = jax.random.split(jax.random.key(seed), 3)
    return {
        "snapshots": draw_snapshots(jax.random.fold_in(seeds[2], 71), 0),
        "sketch": gaussian(seeds[1], (TIMES, K), 1.0, 6.0, ((0, 4),), jnp.float32),
    }


EPS = 1e-06

def scale_rows(value):
    return value * lax.rsqrt(lax.optimization_barrier(jnp.mean(value * value, axis=1, keepdims=True)) + EPS)

def reference(snapshots, sketch):
    sample = scale_rows(jnp.dot(snapshots, sketch, precision=lax.Precision.HIGHEST, preferred_element_type=jnp.float32))
    cosample = scale_rows(lax.dot_general(snapshots, sample, (((0,), (0,)), ((), ())), precision=lax.Precision.HIGHEST, preferred_element_type=jnp.float32))
    refined = scale_rows(jnp.dot(snapshots, cosample, precision=lax.Precision.HIGHEST, preferred_element_type=jnp.float32))
    return (refined, cosample)
```

```python
import functools

import jax
import jax.numpy as jnp
from jax import lax
from jax.experimental import pallas as pl
from jax.experimental.pallas import tpu as pltpu
from jax.sharding import PartitionSpec as P

EPS = 1e-06
F32 = jnp.float32
BF16 = jnp.bfloat16
CHUNKS = 4
LANES = 128
WIDE = 256
LIMIT = pltpu.CompilerParams(vmem_limit_bytes=12 << 20)


def scale_rows(value):
    return value * lax.rsqrt(jnp.mean(value * value, axis=1, keepdims=True) + EPS)


def split(value):
    high = value.astype(BF16)
    return high, (value - high.astype(F32)).astype(BF16)


def dot(left, right):
    return jnp.dot(left, right, preferred_element_type=F32)


def dot3(left, right):
    (lh, ll), (rh, rl) = left, right
    return dot(lh, rh) + dot(ll, rh) + dot(lh, rl)


VMEM = pl.BlockSpec(memory_space=pltpu.VMEM)


def near(value):
    return pltpu.with_memory_space_constraint(value, pltpu.VMEM)


def call(kernel, name, out, args, flops=0, where=None):
    if where is not None:
        args = [where, *args]
    specs = [VMEM] * len(args)
    if where is not None:
        specs[0] = pl.BlockSpec(memory_space=pltpu.SMEM)
    args = [a if where is not None and i == 0 else near(a) for i, a in enumerate(args)]
    shapes = [pltpu.VMEM(shape, dtype) for shape, dtype in out]
    return pl.pallas_call(
        kernel,
        in_specs=specs,
        out_specs=[VMEM] * len(out),
        out_shape=shapes,
        cost_estimate=pl.CostEstimate(flops=flops, bytes_accessed=flops // 256, transcendentals=0),
        name=name,
        compiler_params=LIMIT,
    )(*args)


def split_kernel(value_ref, high_ref, low_ref):
    high_ref[...], low_ref[...] = split(value_ref[...])


def first_kernel(where_ref, block_ref, rh_ref, rl_ref, send_ref, keep_ref, bh_ref, bl_ref):
    i = pl.program_id(0)
    tile = block_ref.shape[0]
    rows = pl.ds(pl.multiple_of(i * tile, tile), tile)
    high, low = split(block_ref[...])
    bh_ref[rows, :] = high
    bl_ref[rows, :] = low
    total = dot3((high, low), (rh_ref[...], rl_ref[...]))
    half = pl.num_programs(0) // 2

    @pl.when(i < half)
    def _():
        send_ref[rows, :] = total

    @pl.when(i >= half)
    def _():
        keep_ref[pl.ds(pl.multiple_of((i - half) * tile, tile), tile), :] = total


def first(where, index, rows, block, right):
    rh, rl = right
    times, cols = rh.shape
    tile = min(rows, LANES)
    steps = rows // tile

    def place(i, w):
        return ((2 * index + jnp.where(i < steps, w[1], w[0])) * steps + lax.rem(i, steps), 0)

    return pl.pallas_call(
        first_kernel,
        grid_spec=pltpu.PrefetchScalarGridSpec(
            num_scalar_prefetch=1,
            grid=(2 * steps,),
            in_specs=[pl.BlockSpec((tile, times), place), VMEM, VMEM],
            out_specs=[VMEM] * 4,
        ),
        out_shape=[
            pltpu.VMEM((rows, cols), F32),
            pltpu.VMEM((rows, cols), F32),
            pltpu.VMEM((2 * rows, times), BF16),
            pltpu.VMEM((2 * rows, times), BF16),
        ],
        cost_estimate=pl.CostEstimate(
            flops=12 * rows * times * cols, bytes_accessed=8 * rows * times, transcendentals=0
        ),
        name="first",
        compiler_params=LIMIT,
    )(where, block, near(rh), near(rl))


def again_kernel(bh_ref, bl_ref, rh_ref, rl_ref, send_ref, keep_ref):
    rows = send_ref.shape[0]
    right = rh_ref[...], rl_ref[...]
    send_ref[...] = dot3((bh_ref[:rows, :], bl_ref[:rows, :]), right)
    keep_ref[...] = dot3((bh_ref[rows:, :], bl_ref[rows:, :]), right)


def again(part, right):
    rows, times = part[0].shape
    cols = right[0].shape[1]
    half = ((rows // 2, cols), F32)
    return call(again_kernel, "again", [half, half], [*part, *right], 6 * rows * times * cols)


def finish_kernel(left_ref, right_ref, out_ref):
    out_ref[...] = scale_rows(left_ref[...] + right_ref[...])


def finish(left, right):
    return call(finish_kernel, "finish", [(left.shape, F32)], [left, right], 8 * left.size)[0]


def back_kernel(slots, *refs):
    if slots:
        where_ref, *refs = refs
    own_ref, other_ref, bh_ref, bl_ref, *acc_ref, out_ref = refs
    sample = jnp.concatenate([other_ref[...], own_ref[...]], axis=0).T
    sample = split(sample)
    times = bh_ref.shape[1]
    wide = min(WIDE, times)
    for at in range(0, times, wide):
        cut = slice(at, at + wide)
        total = dot3(sample, (bh_ref[:, cut], bl_ref[:, cut]))
        if acc_ref:
            total += acc_ref[0][:, cut]
        if not slots:
            out_ref[:, cut] = total
            continue
        width = out_ref.shape[2]
        for part in range(wide // width):
            j = (at // width + part) ^ where_ref[2]
            place = sum(jnp.where(j == s, p, 0) for p, s in enumerate(slots))
            out_ref[place] = total[:, part * width : (part + 1) * width]


def back(where, part, own, other, acc, slots):
    rows, times = part[0].shape
    cols = own.shape[1]
    out = ((len(slots), cols, times // len(slots)) if slots else (cols, times), F32)
    args = [own, other, *part] + ([] if acc is None else [acc])
    return call(
        functools.partial(back_kernel, slots), "back", [out], args, 6 * rows * times * cols,
        where=where if slots else None,
    )[0]


def settle_kernel(a_ref, b_ref, c_ref, d_ref, own_ref, other_ref):
    for left, right, out in ((a_ref, b_ref, own_ref), (c_ref, d_ref, other_ref)):
        value = left[0] + right[0]
        mean = jnp.mean(value * value, axis=0, keepdims=True)
        out[...] = (value * lax.rsqrt(mean + EPS)).T


def settle(a, b, c, d):
    _, cols, rows = a.shape
    return call(settle_kernel, "settle", [((rows, cols), F32)] * 2, [a, b, c, d], 32 * a.size)


def gather_kernel(slots, where_ref, *refs):
    *parts, out_ref, high_ref, low_ref = refs
    rows = parts[0].shape[0]
    for part, j in zip(parts, slots):
        at = pl.ds(pl.multiple_of((where_ref[2] ^ j) * rows, rows), rows)
        value = part[...]
        out_ref[at, :] = value
        high_ref[at, :], low_ref[at, :] = split(value)


def gather(where, parts, slots):
    rows, cols = parts[0].shape
    shape = (rows * len(parts), cols)
    out = [(shape, F32), (shape, BF16), (shape, BF16)]
    return call(functools.partial(gather_kernel, slots), "gather", out, parts, 8 * shape[0] * cols, where=where)


def put_kernel(index, where_ref, own_ref, other_ref, *refs):
    *_, out_ref, sems = refs
    rows = own_ref.shape[0]
    copies = []
    for side, source in enumerate((own_ref, other_ref)):
        at = pl.ds(pl.multiple_of((2 * index + where_ref[side]) * rows, rows), rows)
        copies.append(pltpu.make_async_copy(source, out_ref.at[at, :], sems.at[side]))
    for copy in copies:
        copy.start()
    for copy in copies:
        copy.wait()


def put(where, index, own, other, total, into):
    rows, cols = own.shape
    return pl.pallas_call(
        functools.partial(put_kernel, index),
        in_specs=[pl.BlockSpec(memory_space=pltpu.SMEM), VMEM, VMEM]
        + ([] if into is None else [pl.BlockSpec(memory_space=pl.ANY)]),
        out_specs=pl.BlockSpec(memory_space=pl.ANY),
        out_shape=jax.ShapeDtypeStruct((total, cols), F32),
        scratch_shapes=[pltpu.SemaphoreType.DMA((2,))],
        input_output_aliases={} if into is None else {3: 0},
        cost_estimate=pl.CostEstimate(flops=rows * cols, bytes_accessed=8 * rows * cols, transcendentals=0),
        name="put",
        compiler_params=LIMIT,
    )(where, near(own), near(other), *([] if into is None else [into]))


def swap(value, axis, size, mask):
    return lax.ppermute(value, axis, [(i, i ^ mask) for i in range(size)])


def over_times(size, sent, kept):
    half = kept + swap(sent, "tm", size, 1)
    mask = 2
    while mask * 2 < size:
        half = half + swap(half, "tm", size, mask)
        mask *= 2
    own = finish(half, swap(half, "tm", size, mask))
    return own, swap(own, "tm", size, 1)


def over_space(where, parts, halves, size):
    top = size // 2
    bits = top.bit_length() - 1
    low = [sum(((j >> b) & 1) << (bits - 1 - b) for b in range(bits)) for j in range(top)]
    slots = low + [top + j for j in range(top)]
    acc = None
    for c, (own, other) in enumerate(halves):
        acc = back(where, parts[c], own, other, acc, slots if c == len(halves) - 1 else None)
    one, two = acc[:top], acc[top:]
    for b in range(bits):
        m = one.shape[0] // 2
        one, two = (
            one[:m] + swap(one[m:], "space", size, 1 << b),
            two[:m] + swap(two[m:], "space", size, 1 << (bits - 1 - b)),
        )
    own, other = settle(one, swap(two, "space", size, top), two, swap(one, "space", size, top))
    mine, theirs = {0: own}, {top: other}
    for b in range(bits):
        for held, mask in ((mine, 1 << (bits - 1 - b)), (theirs, 1 << b)):
            held.update({j ^ mask: swap(v, "space", size, mask) for j, v in list(held.items())})
    held = {**mine, **theirs}
    slots = sorted(held)
    return gather(where, [held[j] for j in slots], slots)


def fits(block, size):
    width = block.shape[1] // size
    return size > 2 and size & (size - 1) == 0 and width % LANES == 0


def halve(value):
    return call(split_kernel, "split", [(value.shape, BF16)] * 2, [value], 4 * value.size)


def local(sizes, snapshots, sketch):
    tm, space = sizes
    core = lax.axis_index("tm") & 1
    where = jnp.stack([core, 1 - core, lax.axis_index("space")]).astype(jnp.int32)
    total = snapshots.shape[0]
    rows = total // (2 * CHUNKS)
    right = halve(sketch)
    halves, parts = [], []
    for c in range(CHUNKS):
        sent, kept, *part = first(where, c, rows, snapshots, right)
        halves.append(over_times(tm, sent, kept))
        parts.append(part)
    if fits(snapshots, space):
        cosample, *right = over_space(where, parts, halves, space)
    else:
        acc = None
        for c, (own, other) in enumerate(halves):
            acc = back(where, parts[c], own, other, acc, None)
        cosample = scale_rows(lax.psum(acc, "space").T)
        right = halve(cosample)
    refined = None
    for c in range(CHUNKS):
        own, other = over_times(tm, *again(parts[c], right))
        refined = put(where, c, own, other, total, refined)
    return (refined, cosample)


def solution(mesh):
    return jax.shard_map(
        functools.partial(local, (mesh.shape["tm"], mesh.shape["space"])),
        mesh=mesh,
        in_specs=(P("space", "tm"), P("tm", None)),
        out_specs=(P("space", None), P("tm", None)),
        check_vma=False,
    )
```

```python
import functools

import jax
import jax.numpy as jnp
from jax import lax
from jax.experimental import pallas as pl
from jax.experimental.pallas import tpu as pltpu
from jax.sharding import PartitionSpec as P


EPS = 1e-06
F32 = jnp.float32
BF16 = jnp.bfloat16
SHARES = (2, 2, 2, 1, 1)
LANES = 128
WIDE = 256
TOKEN = (8, LANES)
LIMIT = pltpu.CompilerParams(vmem_limit_bytes=12 << 20)


def scale_rows(value):
    return value * lax.rsqrt(jnp.mean(value * value, axis=1, keepdims=True) + EPS)


def split(value):
    high = value.astype(BF16)
    return high, (value - high.astype(F32)).astype(BF16)


def dot(left, right):
    return jnp.dot(left, right, preferred_element_type=F32)


def dot3(left, right):
    (lh, ll), (rh, rl) = left, right
    return dot(lh, rh) + dot(ll, rh) + dot(lh, rl)


VMEM = pl.BlockSpec(memory_space=pltpu.VMEM)


def near(value):
    return pltpu.with_memory_space_constraint(value, pltpu.VMEM)


def waiting(kernel, at, count):
    return lambda *refs: kernel(*refs[:at], *refs[at + count :])


def call(kernel, out, args, flops=0, where=None, after=()):
    if where is not None:
        args = [where, *args]
    kernel = waiting(kernel, len(args), len(after))
    args = [*args, *after]
    specs = [VMEM] * len(args)
    if where is not None:
        specs[0] = pl.BlockSpec(memory_space=pltpu.SMEM)
    args = [a if where is not None and i == 0 else near(a) for i, a in enumerate(args)]
    shapes = [pltpu.VMEM(shape, dtype) for shape, dtype in out]
    return pl.pallas_call(
        kernel,
        in_specs=specs,
        out_specs=[VMEM] * len(out),
        out_shape=shapes,
        cost_estimate=pl.CostEstimate(flops=flops, bytes_accessed=flops // 256, transcendentals=0),
        compiler_params=LIMIT,
    )(*args)


def split_kernel(value_ref, high_ref, low_ref):
    high_ref[...], low_ref[...] = split(value_ref[...])


def fetch(where_ref, start, block_ref, to_ref, sems):
    rows = to_ref.shape[0] // 2
    return [
        pltpu.make_async_copy(
            block_ref.at[pl.ds(pl.multiple_of(start + where_ref[1 - i] * rows, rows), rows), :],
            to_ref.at[i * rows : (i + 1) * rows, :],
            sems.at[i],
        )
        for i in range(2)
    ]


def first_kernel(opens, starts, *refs):
    where_ref, block_ref, *refs = refs
    if opens:
        right_ref, *refs, now_ref, right, sems, now_sems, right_sem = refs
        send_ref, keep_ref, bh_ref, bl_ref, *next_ref, rh_ref, rl_ref = refs
        here = fetch(where_ref, starts[0], block_ref, now_ref, now_sems)
        load = pltpu.make_async_copy(right_ref, right, right_sem)
        load.start()
        for copy in here:
            copy.start()
    else:
        now_ref, rh_ref, rl_ref, *refs, sems = refs
        send_ref, keep_ref, bh_ref, bl_ref, *next_ref = refs
    ahead = []
    if next_ref:
        ahead = fetch(where_ref, starts[1], block_ref, next_ref[0], sems)
    for copy in ahead:
        copy.start()
    if opens:
        load.wait()
        rh_ref[...], rl_ref[...] = split(right[...])
    rows = send_ref.shape[0]
    tile = min(rows, LANES)
    for i, out_ref in enumerate((send_ref, keep_ref)):
        if opens:
            here[i].wait()
        for at in range(0, rows, tile):
            cut = slice(i * rows + at, i * rows + at + tile)
            high, low = split(now_ref[cut, :])
            bh_ref[cut, :] = high
            bl_ref[cut, :] = low
            out_ref[at : at + tile, :] = dot3((high, low), (rh_ref[...], rl_ref[...]))
    for copy in ahead:
        copy.wait()


def first(where, starts, rows, block, now, right):
    opens = now is None
    ahead = rows[1:2]
    times = block.shape[1]
    cols = (right if opens else right[0]).shape[1]
    out = [((rows[0], cols), F32)] * 2 + [((2 * rows[0], times), BF16)] * 2
    out += [((2 * r, times), F32) for r in ahead]
    out += [((times, cols), BF16)] * 2 if opens else []
    scratch = [pltpu.SemaphoreType.DMA((2,))]
    far = functools.partial(pltpu.with_memory_space_constraint, memory_space=pltpu.HBM)
    specs = [pl.BlockSpec(memory_space=pltpu.SMEM), pl.BlockSpec(memory_space=pl.ANY)]
    if opens:
        args = [far(right)]
        specs += [pl.BlockSpec(memory_space=pl.ANY)]
        scratch = [pltpu.VMEM((2 * rows[0], times), F32), pltpu.VMEM((times, cols), F32)] + scratch
        scratch += [pltpu.SemaphoreType.DMA((2,)), pltpu.SemaphoreType.DMA]
    else:
        args = [near(now), *map(near, right)]
        specs += [VMEM] * 3
    return pl.pallas_call(
        functools.partial(first_kernel, opens, starts),
        in_specs=specs,
        out_specs=[VMEM] * len(out),
        out_shape=[pltpu.VMEM(shape, dtype) for shape, dtype in out],
        scratch_shapes=scratch,
        cost_estimate=pl.CostEstimate(
            flops=12 * rows[0] * times * cols, bytes_accessed=8 * rows[0] * times, transcendentals=0
        ),
        name="first",
        compiler_params=LIMIT,
    )(where, far(block), *args)


def again_kernel(bh_ref, bl_ref, rh_ref, rl_ref, send_ref, keep_ref):
    rows = send_ref.shape[0]
    right = rh_ref[...], rl_ref[...]
    send_ref[...] = dot3((bh_ref[:rows, :], bl_ref[:rows, :]), right)
    keep_ref[...] = dot3((bh_ref[rows:, :], bl_ref[rows:, :]), right)


def again(part, right, after):
    rows, times = part[0].shape
    cols = right[0].shape[1]
    half = ((rows // 2, cols), F32)
    return call(again_kernel, [half, half], [*part, *right], 6 * rows * times * cols, after=after)


def finish_kernel(left_ref, right_ref, out_ref):
    out_ref[...] = scale_rows(left_ref[...] + right_ref[...])


def finish(left, right, after):
    return call(finish_kernel, [(left.shape, F32)], [left, right], 8 * left.size, after=after)[0]


def back_kernel(slots, spans, *refs):
    if slots:
        where_ref, *refs = refs
    samples, (bh_ref, bl_ref, *acc_ref, out_ref) = refs[: len(spans)], refs[len(spans) :]
    rows = slice(spans[0].start, spans[-1].stop)
    sample = split(jnp.concatenate([ref[...] for ref in samples], axis=0).T)
    times = bh_ref.shape[1]
    wide = min(WIDE, times)
    for at in range(0, times, wide):
        cut = slice(at, at + wide)
        total = dot3(sample, (bh_ref[rows, cut], bl_ref[rows, cut]))
        if acc_ref:
            total += acc_ref[0][:, cut]
        if not slots:
            out_ref[:, cut] = total
            continue
        width = out_ref.shape[2]
        for part in range(wide // width):
            j = (at // width + part) ^ where_ref[2]
            place = sum(jnp.where(j == s, p, 0) for p, s in enumerate(slots))
            out_ref[place] = total[:, part * width : (part + 1) * width]


def back(where, part, samples, spans, acc, slots=None):
    times = part[0].shape[1]
    cols = samples[0].shape[1]
    rows = sum(len(range(s.start, s.stop)) for s in spans)
    out = ((len(slots), cols, times // len(slots)) if slots else (cols, times), F32)
    args = [*samples, *part] + ([] if acc is None else [acc])
    return call(
        functools.partial(back_kernel, slots, spans), [out], args, 6 * rows * times * cols,
        where=where if slots else None,
    )[0]


def settle_kernel(a_ref, b_ref, c_ref, d_ref, own_ref, other_ref):
    for left, right, out in ((a_ref, b_ref, own_ref), (c_ref, d_ref, other_ref)):
        value = left[0] + right[0]
        mean = jnp.mean(value * value, axis=0, keepdims=True)
        out[...] = (value * lax.rsqrt(mean + EPS)).T


def settle(a, b, c, d):
    _, cols, rows = a.shape
    return call(settle_kernel, [((rows, cols), F32)] * 2, [a, b, c, d], 32 * a.size)


def gather_kernel(slots, where_ref, *refs):
    *parts, high_ref, low_ref = refs
    rows = parts[0].shape[0]
    for part, j in zip(parts, slots):
        at = pl.ds(pl.multiple_of((where_ref[2] ^ j) * rows, rows), rows)
        high_ref[at, :], low_ref[at, :] = split(part[...])


def gather(where, parts, slots):
    rows, cols = parts[0].shape
    shape = (rows * len(parts), cols)
    out = [(shape, BF16), (shape, BF16)]
    return call(functools.partial(gather_kernel, slots), out, parts, 8 * shape[0] * cols, where=where)


def emit_kernel(slots, where_ref, *refs):
    parts, (out_ref, done_ref, sems) = refs[: len(slots)], refs[len(slots) :]
    rows = parts[0].shape[0]
    copies = []
    for i, j in enumerate(slots):
        at = pl.ds(pl.multiple_of((where_ref[2] ^ j) * rows, rows), rows)
        copies.append(pltpu.make_async_copy(parts[i], out_ref.at[at, :], sems.at[i]))
    for copy in copies:
        copy.start()
    done_ref[...] = jnp.zeros_like(done_ref)
    for copy in copies:
        copy.wait()


def emit(where, parts, slots, after):
    rows, cols = parts[0].shape
    return pl.pallas_call(
        waiting(functools.partial(emit_kernel, slots), 1 + len(parts), len(after)),
        in_specs=[pl.BlockSpec(memory_space=pltpu.SMEM)] + [VMEM] * (len(parts) + len(after)),
        out_specs=[pl.BlockSpec(memory_space=pl.ANY), VMEM],
        out_shape=[pltpu.HBM((rows * len(parts), cols), F32), pltpu.VMEM(TOKEN, F32)],
        scratch_shapes=[pltpu.SemaphoreType.DMA((len(parts),))],
        cost_estimate=pl.CostEstimate(flops=rows * cols, bytes_accessed=8 * rows * cols, transcendentals=0),
        name="emit",
        compiler_params=LIMIT,
    )(where, *map(near, (*parts, *after)))


def put_kernel(start, sides, where_ref, *refs):
    parts, (*_, out_ref, done_ref, sems) = refs[: len(sides)], refs[len(sides) :]
    rows = parts[0].shape[0]
    copies = []
    for i, side in enumerate(sides):
        at = pl.ds(pl.multiple_of(start + where_ref[side] * rows, rows), rows)
        copies.append(pltpu.make_async_copy(parts[i], out_ref.at[at, :], sems.at[i]))
    for copy in copies:
        copy.start()
    done_ref[...] = jnp.zeros_like(done_ref)
    for copy in copies:
        copy.wait()


def put(where, start, sides, parts, total, into):
    rows, cols = parts[0].shape
    return pl.pallas_call(
        functools.partial(put_kernel, start, sides),
        in_specs=[pl.BlockSpec(memory_space=pltpu.SMEM)]
        + [VMEM] * len(parts)
        + ([] if into is None else [pl.BlockSpec(memory_space=pl.ANY)]),
        out_specs=[pl.BlockSpec(memory_space=pl.ANY), VMEM],
        out_shape=[pltpu.HBM((total, cols), F32), pltpu.VMEM(TOKEN, F32)],
        scratch_shapes=[pltpu.SemaphoreType.DMA((len(parts),))],
        input_output_aliases={} if into is None else {1 + len(parts): 0},
        cost_estimate=pl.CostEstimate(flops=rows * cols, bytes_accessed=8 * rows * cols, transcendentals=0),
        name="put",
        compiler_params=LIMIT,
    )(where, *map(near, parts), *([] if into is None else [into]))


def swap(value, axis, size, mask):
    return lax.ppermute(value, axis, [(i, i ^ mask) for i in range(size)])


def across(size, sent, kept):
    half = kept + swap(sent, "tm", size, 1)
    mask = 2
    while mask * 2 < size:
        half = half + swap(half, "tm", size, mask)
        mask *= 2
    return half, swap(half, "tm", size, mask)


def over_space(acc, size):
    top = size // 2
    bits = top.bit_length() - 1
    one, two = acc[:top], acc[top:]
    for b in range(bits):
        m = one.shape[0] // 2
        got = swap(one[m:], "space", size, 1 << b), swap(two[m:], "space", size, 1 << (bits - 1 - b))
        got = lax.optimization_barrier(got)
        one, two = one[:m] + got[0], two[:m] + got[1]
    got = lax.optimization_barrier((swap(two, "space", size, top), swap(one, "space", size, top)))
    own, other = settle(one, got[0], two, got[1])
    mine, theirs = {0: own}, {top: other}
    for b in range(bits):
        for held, mask in ((mine, 1 << (bits - 1 - b)), (theirs, 1 << b)):
            held.update({j ^ mask: swap(v, "space", size, mask) for j, v in list(held.items())})
    return {**mine, **theirs}


def order(size):
    top = size // 2
    bits = top.bit_length() - 1
    low = [sum(((j >> b) & 1) << (bits - 1 - b) for b in range(bits)) for j in range(top)]
    return low + [top + j for j in range(top)]


def fits(block, size):
    width = block.shape[1] // size
    return size > 2 and size & (size - 1) == 0 and width % LANES == 0


def halve(value):
    return call(split_kernel, [(value.shape, BF16)] * 2, [value], 4 * value.size)


def local(sizes, snapshots, sketch):
    tm, space = sizes
    core = lax.axis_index("tm") & 1
    where = jnp.stack([core, 1 - core, lax.axis_index("space")]).astype(jnp.int32)
    total = snapshots.shape[0]
    unit = total // (2 * sum(SHARES))
    rows = [unit * share for share in SHARES]
    starts = [2 * sum(rows[:c]) for c in range(len(rows))]
    chunks = range(len(rows))
    spread = fits(snapshots, space)

    parts, sums, now, right = [], [], None, sketch
    for c in chunks:
        sent, kept, *part = first(where, starts[c : c + 2], rows[c : c + 2], snapshots, now, right)
        if c == 0:
            *part, rh, rl = part
            right = rh, rl
        parts.append(part[:2])
        now = part[-1]
        sums.append(across(tm, sent, kept))
    acc, after = None, []
    for c in chunks:
        far, near_ = slice(0, rows[c]), slice(rows[c], 2 * rows[c])
        own = finish(*sums[c], after)
        other = swap(own, "tm", tm, 1)
        if c < chunks[-1]:
            acc = back(where, parts[c], (other, own), (far, near_), acc)
            after = [acc]
        else:
            acc = back(where, parts[c], (own,), (near_,), acc)
            acc = back(where, parts[c], (other,), (far,), acc, order(space) if spread else None)
    if spread:
        held = over_space(acc, space)
        slots = sorted(held)
        right = gather(where, [held[j] for j in slots], slots)
    else:
        cosample = scale_rows(lax.psum(acc, "space").T)
        right = halve(cosample)
    sums = []
    for c in chunks:
        halves = again(parts[c], right, [])
        sums.append(across(tm, *halves))
    after, token = [], []
    if spread:
        cosample, *token = emit(where, [held[j] for j in slots], slots, [])
    refined = None
    for c in chunks:
        own = finish(*sums[c], after)
        other = swap(own, "tm", tm, 1)
        refined, ready = put(where, starts[c], (0, 1), (own, other), total, refined)
        after = [ready, *token]
    return (refined, cosample)


def solution(mesh):
    tm, space = mesh.shape["tm"], mesh.shape["space"]

    def body(snapshots, sketch):
        return local((tm, space), snapshots, sketch)

    return jax.shard_map(
        body,
        mesh=mesh,
        in_specs=(P("space", "tm"), P("tm", None)),
        out_specs=(P("space", None), P("tm", None)),
        check_vma=False,
    )
```
